32 devices in a mesh: groups: 2 (over y), det: 4 (over z), blk: 2 (over x), sub: 2 (over core).
Axes of the slice: x: 2, y: 2, z: 4, core: 2. Of those that a mesh axis runs over, the one named last changes fastest.
Arguments:
- tod: float32 [256, 4, 1024], P(('groups', 'det'), None, ('blk', 'sub')), parts along dimension 0, may hold values from -30 to 30
- pixels: int32 [256, 4, 1024], P('groups', 'det', ('blk', 'sub')), parts along dimension 0, may hold values from 0 to 3071
- span_block: int32 [8, 8], P('groups', ('blk', 'sub')), parts along dimension 0, may hold values from 0 to 7
- weight_class: int32 [256], P('groups'), parts along dimension 0, may hold values from 0 to 7
- class_weight: float32 [16], P('groups'), parts along dimension 0, may hold values from 0.25 to 4
Outputs:
- signal_sum: float32 [16, 3072], P(('groups', 'blk'), ('det', 'sub')), parts along dimension 0
- weight_sum: float32 [16, 3072], P(('groups', 'blk'), ('det', 'sub')), parts along dimension 0
- hit_count: float32 [16, 3072], P(('groups', 'blk'), ('det', 'sub')), parts along dimension 0
The draws below stay inside these ranges and needn't reach their ends.
There are 2 independent parts, one for each index of `groups`. The reference program is written for one: setup_inputs(seed, part) draws one part's arguments, and reference() takes and returns one part's arrays. A program takes and returns all parts, laid end to end along the dimension named above; each array names one. Nothing has to cross between parts.
All inputs are finite; a program needn't handle non-finite values.
Results may differ from the reference program's by a relative error of at most 0.005.
Values sent between devices are 32-bit elements; how exact they have to be, the bound alone decides.
A program may use at most 64 MiB of HBM per device.

```python
import math
import jax
import jax.numpy as jnp
from jax import lax

BLOCK_PIX = 3072
SPAN = 128
NCLASS = 8
NDET = 128
NSEG = 4
SEG = 1024
NCHUNK = 8
NBLOCKS = 8


def shared_integers(key):
    key_base = jax.random.fold_in(key, 29)
    key_perm, key_first, key_second, key_class, key_one, key_two = jax.random.split(key_base, 6)
    block_order = jax.random.permutation(key_perm, NBLOCKS).astype(jnp.int32)
    first_pick = jax.random.randint(key_first, (NSEG, NCHUNK), 0, NBLOCKS, dtype=jnp.int32)
    second_pick = jax.random.randint(key_second, (NSEG, NCHUNK), 0, NBLOCKS, dtype=jnp.int32)
    span_block = block_order[jnp.minimum(first_pick, second_pick)].astype(jnp.int32)
    weight_class = jax.random.randint(key_class, (NDET,), 0, NCLASS, dtype=jnp.int32)
    pick_one = jax.random.randint(key_one, (NDET, NSEG, SEG), 0, BLOCK_PIX, dtype=jnp.int32)
    pick_two = jax.random.randint(key_two, (NDET, NSEG, SEG), 0, BLOCK_PIX, dtype=jnp.int32)
    ranked = jnp.minimum(pick_one, pick_two)
    blocks = jnp.repeat(span_block, SPAN, axis=1)
    shift_block = blocks[None] * 977 * BLOCK_PIX // 3072
    shift_class = weight_class[:, None, None] * 131 * BLOCK_PIX // 3072
    pixels = ((ranked + shift_block + shift_class) % BLOCK_PIX).astype(jnp.int32)
    return (span_block, weight_class, pixels)


def draw_pixels(key, part):
    return shared_integers(key)[2]


def draw_span_block(key, part):
    return shared_integers(key)[0]


def draw_weight_class(key, part):
    return shared_integers(key)[1]


def draw_tod(key, part):
    base = jax.random.fold_in(key, 17)
    key_gain, key_common, key_noise = jax.random.split(base, 3)
    gains = jax.random.uniform(key_gain, (NDET, 1, 1), jnp.float32, 0.5, 1.5)
    common = 3.0 * jax.random.normal(key_common, (1, NSEG, SEG), jnp.float32)
    noise = jax.random.normal(key_noise, (NDET, NSEG, SEG), jnp.float32)
    return jnp.clip(gains * common + noise, -30.0, 30.0)


def setup_inputs(seed: int = 0, part: int = 0) -> dict:
    key_list = jax.random.split(jax.random.key(seed), 6)
    part_splits = jax.random.split(jax.random.fold_in(key_list[5], part), 6)
    tod = draw_tod(jax.random.fold_in(jax.random.fold_in(key_list[5], part), 71), part)
    pixels = draw_pixels(jax.random.fold_in(jax.random.fold_in(key_list[5], part), 71), part)
    span_block = draw_span_block(jax.random.fold_in(jax.random.fold_in(key_list[5], part), 71), part)
    weight_class = draw_weight_class(jax.random.fold_in(jax.random.fold_in(key_list[5], part), 71), part)
    class_weight = jnp.clip(jnp.exp(jax.random.uniform(part_splits[4], (NCLASS,), jnp.float32, math.log(0.25), math.log(4.0))), 0.25, 4.0)
    return {"tod": tod, "pixels": pixels, "span_block": span_block, "weight_class": weight_class, "class_weight": class_weight}


def reference(tod, pixels, span_block, weight_class, class_weight):
    weight = class_weight[weight_class]
    total = jnp.sum(weight)
    common = jnp.sum(weight[:, None, None] * tod, axis=0) / total
    value = (weight[:, None, None] * (tod - common[None])).astype(jnp.bfloat16)
    value = value.astype(jnp.float32)
    weight_low = lax.optimization_barrier(weight.astype(jnp.bfloat16)).astype(jnp.float32)
    blocks = jnp.repeat(span_block, SPAN, axis=1)
    pixel = (blocks[None] * BLOCK_PIX + pixels).astype(jnp.int32).reshape(-1)
    count = NBLOCKS * BLOCK_PIX
    signal_sum = jax.ops.segment_sum(value.reshape(-1), pixel, num_segments=count)
    weight_full = jnp.broadcast_to(weight_low[:, None, None], tod.shape).reshape(-1)
    weight_sum = jax.ops.segment_sum(weight_full, pixel, num_segments=count)
    hit_count = jax.ops.segment_sum(jnp.ones(pixel.shape, jnp.float32), pixel, num_segments=count)
    return (signal_sum.reshape(NBLOCKS, BLOCK_PIX), weight_sum.reshape(NBLOCKS, BLOCK_PIX), hit_count.reshape(NBLOCKS, BLOCK_PIX))
```

```python
import functools

import jax
import jax.numpy as jnp
from jax import lax
from jax.experimental import pallas as pl
from jax.experimental.pallas import tpu as pltpu
from jax.sharding import PartitionSpec as P

BLOCK_PIX = 3072
SPAN = 128
BLK_OWN = 4
TILE = 8
PACK = 16
MESH = pl.DeviceIdType.MESH


def kernel(
    sizes,
    tod_hbm,
    pix_hbm,
    class_ref,
    class_weight_ref,
    span_block_ref,
    signal_ref,
    weight_ref,
    hits_ref,
    tod_in,
    pix_in,
    stage,
    tod_all,
    high_ref,
    low_ref,
    weight_rows,
    value_ref,
    early_out,
    early_in,
    late_out,
    late_in,
    load_sem,
    tod_send,
    tod_recv,
    early_send,
    early_recv,
    late_send,
    late_recv,
):
    ndet, nblk, nsub, spans, lanes, rows = sizes
    peers = ndet * nsub
    total_peers = peers * nblk
    mine = tod_hbm.shape[0]
    detectors = ndet * mine
    classes = class_weight_ref.shape[0]
    det = lax.axis_index("det")
    blk = lax.axis_index("blk")
    sub = lax.axis_index("sub")
    load_tod = pltpu.make_async_copy(tod_hbm, tod_in, load_sem.at[0])
    load_pix = pltpu.make_async_copy(pix_hbm, pix_in, load_sem.at[1])
    load_tod.start()
    load_pix.start()
    others = [
        (db, dd, ds)
        for dd in range(ndet)
        for db in range(nblk)
        for ds in range(nsub)
        if (db, dd, ds) != (0, 0, 0)
    ]

    def target(offset):
        db, dd, ds = offset
        return {
            "det": lax.rem(det + dd, ndet),
            "blk": lax.rem(blk + db, nblk),
            "sub": lax.rem(sub + ds, nsub),
        }

    barrier = pltpu.get_barrier_semaphore()
    for offset in others:
        pl.semaphore_signal(barrier, inc=1, device_id=target(offset), device_id_type=MESH)

    part = mine * spans
    load_tod.wait()
    for seg in range(ndet):
        for span in range(spans):
            stage[seg, pl.ds(span, mine, spans), :] = tod_in[:, seg, span * SPAN : (span + 1) * SPAN]
    pl.semaphore_wait(barrier, len(others))
    for step in range(1, ndet):
        seg = lax.rem(det + step, ndet)
        pltpu.make_async_remote_copy(
            src_ref=stage.at[seg],
            dst_ref=tod_all.at[det],
            send_sem=tod_send,
            recv_sem=tod_recv,
            device_id={"det": seg},
            device_id_type=MESH,
        ).start()
    tod_all[det] = stage[det]

    picked = jnp.zeros((1, detectors), jnp.float32)
    for c in range(classes):
        picked = jnp.where(class_ref[...] == c, class_weight_ref[c], picked)
    total = jnp.sum(picked, axis=1, keepdims=True)
    turned = jnp.transpose(jnp.broadcast_to(picked, (SPAN, detectors)))
    for span in range(spans):
        weight_rows[pl.ds(span, detectors, spans), :] = turned

    load_pix.wait()
    pixel = pix_in[...].astype(jnp.float32)
    high = jnp.floor((pixel + 0.5) * (1.0 / lanes))
    high_ref[...] = high
    low_ref[...] = pixel - high * lanes

    height = peers * TILE
    low_tiles = -(-lanes // PACK)

    def iota(tile):
        return lax.broadcasted_iota(jnp.int32, (PACK, SPAN), 0) + tile * PACK

    def to_low(x):
        return x.astype(jnp.float32).astype(jnp.bfloat16)

    low_ids = [to_low(iota(t)) for t in range(SPAN // PACK)]
    early_ids = []
    late_ids = [[] for _ in range(spans)]
    for t in range(height // PACK):
        row = iota(t)
        peer = row // TILE
        within = row % TILE
        kind = jnp.where(within < rows, within, within - rows)
        early_ids.append(to_low(jnp.where(within < 2 * rows, peer * rows + kind, -1)))
        for span in range(spans):
            inner = within - span * rows
            valid = jnp.logical_and(inner >= 0, inner < rows)
            late_ids[span].append(to_low(jnp.where(valid, peer * rows + inner, -1)))
    is_weight = to_low(jnp.where(iota(0) % TILE < rows, 1, 0)) > 0.5
    one = jnp.ones((PACK, SPAN), jnp.bfloat16)
    zero = jnp.zeros((PACK, SPAN), jnp.bfloat16)

    def spread(ref, row):
        return jnp.broadcast_to(ref[pl.ds(row, 1), :], (PACK, SPAN)).astype(jnp.bfloat16)

    def hot(ids, where, filled):
        return jnp.concatenate([jnp.where(i == where, filled, zero) for i in ids], axis=0)

    chunk = 8

    def contract(left, right):
        return lax.dot_general(
            jnp.concatenate(left, axis=1),
            jnp.concatenate(right, axis=1),
            (((1,), (1,)), ((), ())),
            preferred_element_type=jnp.float32,
        )

    def early_step(i, sums):
        base = pl.multiple_of(i * chunk * spans, TILE)
        new = []
        for span in range(spans):
            left, right = [], []
            for d in range(chunk):
                r = base + d * spans + span
                right.append(hot(low_ids, spread(low_ref, r), one))
                filled = jnp.where(is_weight, spread(weight_rows, r), one)
                left.append(hot(early_ids, spread(high_ref, r), filled))
            new.append(sums[span] + contract(left, right))
        return tuple(new)

    start = tuple(jnp.zeros((height, SPAN), jnp.float32) for _ in range(spans))
    sums = lax.fori_loop(0, detectors // chunk, early_step, start)
    label_row = lax.broadcasted_iota(jnp.int32, (TILE, SPAN), 0) == 2 * rows
    for span in range(spans):
        label = span_block_ref[det, span].astype(jnp.float32)
        for p in range(peers):
            tile = sums[span][p * TILE : (p + 1) * TILE]
            early_out[p, span] = jnp.where(label_row, label, tile)

    slot_of = {offset: n for n, offset in enumerate(others)}

    def send(source, landing, send_sem, recv_sem):
        for offset in others:
            to = target(offset)
            pltpu.make_async_remote_copy(
                src_ref=source.at[to["det"] * nsub + to["sub"]],
                dst_ref=landing.at[slot_of[offset]],
                send_sem=send_sem,
                recv_sem=recv_sem,
                device_id=to,
                device_id_type=MESH,
            ).start()

    own_place = det * nsub + sub
    remote = len(others)

    tod_gone = stage.at[pl.ds(0, ndet - 1)]
    pltpu.make_async_copy(tod_gone, tod_all.at[pl.ds(0, ndet - 1)], tod_recv).wait()
    send(early_out, early_in, early_send, early_recv)

    period = TILE
    folded = jnp.zeros((period, SPAN), jnp.float32)
    for q in range(ndet):
        weighted = tod_all[q] * weight_rows[q * part : (q + 1) * part]
        for k in range(part // period):
            folded = folded + weighted[k * period : (k + 1) * period]
    shift = spans
    while shift < period:
        folded = folded + pltpu.roll(folded, shift, 0)
        shift *= 2
    common = folded / total
    for q in range(ndet):
        piece = slice(q * part, (q + 1) * part)
        repeated = jnp.concatenate([common] * (part // period), axis=0)
        value_ref[piece] = weight_rows[piece] * (tod_all[q] - repeated)

    def late_step(i, total_sum):
        base = pl.multiple_of(i * chunk * spans, TILE)
        for span in range(spans):
            left, right = [], []
            for d in range(chunk):
                r = base + d * spans + span
                right.append(hot(low_ids, spread(low_ref, r), one))
                left.append(hot(late_ids[span], spread(high_ref, r), spread(value_ref, r)))
            total_sum = total_sum + contract(left, right)
        return total_sum

    late = lax.fori_loop(0, detectors // chunk, late_step, jnp.zeros((height, SPAN), jnp.float32))
    for p in range(peers):
        late_out[p] = late[p * TILE : (p + 1) * TILE]
    send(late_out, late_in, late_send, late_recv)
    late_in[remote] = late_out[own_place]
    early_in[remote] = early_out[own_place]

    pltpu.make_async_copy(early_in.at[pl.ds(0, remote)], early_in.at[pl.ds(0, remote)], early_recv).wait()
    first = (blk * BLK_OWN).astype(jnp.float32)

    def gather_early(n, acc):
        acc = list(acc)
        for span in range(spans):
            tile = early_in[n, span]
            label = jnp.broadcast_to(early_in[n, span, pl.ds(2 * rows, 1), :], (TILE, SPAN))
            for b in range(BLK_OWN):
                acc[b] = acc[b] + jnp.where(label == first + b, tile, 0.0)
        return tuple(acc)

    within = lax.broadcasted_iota(jnp.int32, (TILE, SPAN), 0)

    def gather_late(n, acc):
        label = jnp.broadcast_to(early_in[n, 0, pl.ds(2 * rows, 1), :], (TILE, SPAN))
        for span in range(1, spans):
            other = jnp.broadcast_to(early_in[n, span, pl.ds(2 * rows, 1), :], (TILE, SPAN))
            label = jnp.where(within < span * rows, label, other)
        tile = late_in[n]
        return tuple(
            acc[b] + jnp.where(label == first + b, tile, 0.0) for b in range(BLK_OWN)
        )

    def over_slots(step):
        acc = tuple(jnp.zeros((TILE, SPAN), jnp.float32) for _ in range(BLK_OWN))
        if total_peers <= 16:
            for n in range(total_peers):
                acc = step(n, acc)
            return acc
        return lax.fori_loop(0, total_peers, step, acc)

    acc = over_slots(gather_early)
    for b in range(BLK_OWN):
        for r in range(rows):
            at = slice(r * lanes, (r + 1) * lanes)
            weight_ref[b : b + 1, at] = acc[b][r : r + 1, :lanes]
            hits_ref[b : b + 1, at] = acc[b][rows + r : rows + r + 1, :lanes]

    pltpu.make_async_copy(late_in.at[pl.ds(0, remote)], late_in.at[pl.ds(0, remote)], late_recv).wait()
    acc = over_slots(gather_late)
    for b in range(BLK_OWN):
        for r in range(rows):
            line = acc[b][r : r + 1]
            for span in range(1, spans):
                line = line + acc[b][span * rows + r : span * rows + r + 1]
            signal_ref[b : b + 1, r * lanes : (r + 1) * lanes] = line[:, :lanes]

    pltpu.make_async_copy(tod_gone, tod_all.at[pl.ds(0, ndet - 1)], tod_send).wait()
    pltpu.make_async_copy(early_in.at[pl.ds(0, remote)], early_in.at[pl.ds(0, remote)], early_send).wait()
    pltpu.make_async_copy(late_in.at[pl.ds(0, remote)], late_in.at[pl.ds(0, remote)], late_send).wait()


def on_device(tod, pixels, span_block, weight_class, class_weight):
    ndet, nblk, nsub = (lax.axis_size(a) for a in ("det", "blk", "sub"))
    mine, segments, samples = tod.shape
    detectors = pixels.shape[0]
    spans = samples // SPAN
    peers = ndet * nsub
    slots = peers * nblk
    width = BLOCK_PIX // peers
    lanes = next(n for n in range(SPAN, 0, -1) if width % n == 0)
    rows = width // lanes
    assert segments == ndet and detectors == ndet * mine
    assert TILE % spans == 0 and rows * spans <= TILE and 2 * rows < TILE
    flat = (detectors * spans, SPAN)
    out = jax.ShapeDtypeStruct((BLK_OWN, width), jnp.float32)
    vmem = pl.BlockSpec(memory_space=pltpu.VMEM)
    smem = pl.BlockSpec(memory_space=pltpu.SMEM)
    hbm = pl.BlockSpec(memory_space=pl.ANY)
    f32 = jnp.float32
    dma = pltpu.SemaphoreType.DMA
    return pl.pallas_call(
        functools.partial(kernel, (ndet, nblk, nsub, spans, lanes, rows)),
        out_shape=(out, out, out),
        in_specs=[hbm, hbm, vmem, smem, smem],
        out_specs=(vmem, vmem, vmem),
        scratch_shapes=[
            pltpu.VMEM(tod.shape, f32),
            pltpu.VMEM(flat, jnp.int32),
            pltpu.VMEM((ndet, mine * spans, SPAN), f32),
            pltpu.VMEM((ndet, mine * spans, SPAN), f32),
            pltpu.VMEM(flat, f32),
            pltpu.VMEM(flat, f32),
            pltpu.VMEM(flat, f32),
            pltpu.VMEM(flat, f32),
            pltpu.VMEM((peers, spans, TILE, SPAN), f32),
            pltpu.VMEM((slots, spans, TILE, SPAN), f32),
            pltpu.VMEM((peers, TILE, SPAN), f32),
            pltpu.VMEM((slots, TILE, SPAN), f32),
            dma((2,)),
            dma,
            dma,
            dma,
            dma,
            dma,
            dma,
        ],
        compiler_params=pltpu.CompilerParams(collective_id=0, has_side_effects=True),
    )(
        tod,
        pixels.reshape(flat),
        weight_class.reshape(1, detectors),
        class_weight,
        span_block,
    )


def solution(mesh):
    placed = (
        P(("groups", "det"), None, ("blk", "sub")),
        P("groups", "det", ("blk", "sub")),
        P("groups", ("blk", "sub")),
        P("groups"),
        P("groups"),
    )
    sliced = P(("groups", "blk"), ("det", "sub"))
    return jax.shard_map(
        on_device,
        mesh=mesh,
        in_specs=placed,
        out_specs=(sliced, sliced, sliced),
        check_vma=False,
    )
```

```python
import functools

import jax
import jax.numpy as jnp
from jax import lax
from jax.experimental import pallas as pl
from jax.experimental.pallas import tpu as pltpu
from jax.sharding import PartitionSpec as P

BLOCK_PIX = 3072
SPAN = 128
BLK_OWN = 4
TILE = 8
PACK = 16
MESH = pl.DeviceIdType.MESH


def kernel(
    sizes,
    tod_hbm,
    pix_hbm,
    class_ref,
    class_weight_ref,
    span_block_ref,
    out_ref,
    tod_in,
    pix_in,
    stage,
    tod_all,
    high_ref,
    low_ref,
    weight_rows,
    value_ref,
    early_out,
    early_in,
    late_out,
    late_in,
    load_sem,
    tod_send,
    tod_recv,
    early_send,
    early_recv,
    late_send,
    late_recv,
):
    ndet, nblk, nsub, spans, lanes, rows = sizes
    peers = ndet * nsub
    total_peers = peers * nblk
    mine = tod_hbm.shape[0]
    detectors = ndet * mine
    classes = class_weight_ref.shape[0]
    det = lax.axis_index("det")
    blk = lax.axis_index("blk")
    sub = lax.axis_index("sub")
    load_tod = pltpu.make_async_copy(tod_hbm, tod_in, load_sem.at[0])
    load_pix = pltpu.make_async_copy(pix_hbm, pix_in, load_sem.at[1])
    load_tod.start()
    load_pix.start()
    others = [
        (db, dd, ds)
        for dd in range(ndet)
        for db in range(nblk)
        for ds in range(nsub)
        if (db, dd, ds) != (0, 0, 0)
    ]

    def target(offset):
        db, dd, ds = offset
        return {
            "det": lax.rem(det + dd, ndet),
            "blk": lax.rem(blk + db, nblk),
            "sub": lax.rem(sub + ds, nsub),
        }

    barrier = pltpu.get_barrier_semaphore()
    for offset in others:
        pl.semaphore_signal(barrier, inc=1, device_id=target(offset), device_id_type=MESH)

    part = mine * spans
    load_tod.wait()
    for seg in range(ndet):
        for span in range(spans):
            stage[seg, pl.ds(span, mine, spans), :] = tod_in[:, seg, span * SPAN : (span + 1) * SPAN]
    pl.semaphore_wait(barrier, len(others))
    for step in range(1, ndet):
        seg = lax.rem(det + step, ndet)
        pltpu.make_async_remote_copy(
            src_ref=stage.at[seg],
            dst_ref=tod_all.at[det],
            send_sem=tod_send,
            recv_sem=tod_recv,
            device_id={"det": seg},
            device_id_type=MESH,
        ).start()
    tod_all[det] = stage[det]

    picked = jnp.zeros((1, detectors), jnp.float32)
    for c in range(classes):
        picked = jnp.where(class_ref[...] == c, class_weight_ref[c], picked)
    total = jnp.sum(picked, axis=1, keepdims=True)
    turned = jnp.transpose(jnp.broadcast_to(picked, (SPAN, detectors)))
    for span in range(spans):
        weight_rows[pl.ds(span, detectors, spans), :] = turned

    load_pix.wait()
    pixel = pix_in[...].astype(jnp.float32)
    high = jnp.floor((pixel + 0.5) * (1.0 / lanes))
    high_ref[...] = high
    low_ref[...] = pixel - high * lanes

    height = peers * TILE
    low_tiles = -(-lanes // PACK)

    def iota(tile):
        return lax.broadcasted_iota(jnp.int32, (PACK, SPAN), 0) + tile * PACK

    def to_low(x):
        return x.astype(jnp.float32).astype(jnp.bfloat16)

    low_ids = [to_low(iota(t)) for t in range(SPAN // PACK)]
    early_ids = []
    late_ids = [[] for _ in range(spans)]
    for t in range(height // PACK):
        row = iota(t)
        peer = row // TILE
        within = row % TILE
        kind = jnp.where(within < rows, within, within - rows)
        early_ids.append(to_low(jnp.where(within < 2 * rows, peer * rows + kind, -1)))
        for span in range(spans):
            inner = within - span * rows
            valid = jnp.logical_and(inner >= 0, inner < rows)
            late_ids[span].append(to_low(jnp.where(valid, peer * rows + inner, -1)))
    is_weight = to_low(jnp.where(iota(0) % TILE < rows, 1, 0)) > 0.5
    one = jnp.ones((PACK, SPAN), jnp.bfloat16)
    zero = jnp.zeros((PACK, SPAN), jnp.bfloat16)

    def spread(ref, row):
        return jnp.broadcast_to(ref[pl.ds(row, 1), :], (PACK, SPAN)).astype(jnp.bfloat16)

    def hot(ids, where, filled):
        return jnp.concatenate([jnp.where(i == where, filled, zero) for i in ids], axis=0)

    chunk = 8

    def contract(left, right):
        return lax.dot_general(
            jnp.concatenate(left, axis=1),
            jnp.concatenate(right, axis=1),
            (((1,), (1,)), ((), ())),
            preferred_element_type=jnp.float32,
        )

    def early_step(i, sums):
        base = pl.multiple_of(i * chunk * spans, TILE)
        new = []
        for span in range(spans):
            left, right = [], []
            for d in range(chunk):
                r = base + d * spans + span
                right.append(hot(low_ids, spread(low_ref, r), one))
                filled = jnp.where(is_weight, spread(weight_rows, r), one)
                left.append(hot(early_ids, spread(high_ref, r), filled))
            new.append(sums[span] + contract(left, right))
        return tuple(new)

    start = tuple(jnp.zeros((height, SPAN), jnp.float32) for _ in range(spans))
    sums = lax.fori_loop(0, detectors // chunk, early_step, start)
    label_row = lax.broadcasted_iota(jnp.int32, (TILE, SPAN), 0) == 2 * rows
    for span in range(spans):
        label = span_block_ref[span, det].astype(jnp.float32)
        for p in range(peers):
            tile = sums[span][p * TILE : (p + 1) * TILE]
            early_out[p, span] = jnp.where(label_row, label, tile)

    slot_of = {offset: n for n, offset in enumerate(others)}

    def send(source, landing, send_sem, recv_sem):
        for offset in others:
            to = target(offset)
            pltpu.make_async_remote_copy(
                src_ref=source.at[to["det"] * nsub + to["sub"]],
                dst_ref=landing.at[slot_of[offset]],
                send_sem=send_sem,
                recv_sem=recv_sem,
                device_id=to,
                device_id_type=MESH,
            ).start()

    own_place = det * nsub + sub
    remote = len(others)

    tod_gone = stage.at[pl.ds(0, ndet - 1)]
    pltpu.make_async_copy(tod_gone, tod_all.at[pl.ds(0, ndet - 1)], tod_recv).wait()
    send(early_out, early_in, early_send, early_recv)

    period = TILE
    folded = jnp.zeros((period, SPAN), jnp.float32)
    for q in range(ndet):
        weighted = tod_all[q] * weight_rows[q * part : (q + 1) * part]
        for k in range(part // period):
            folded = folded + weighted[k * period : (k + 1) * period]
    shift = spans
    while shift < period:
        folded = folded + pltpu.roll(folded, shift, 0)
        shift *= 2
    common = folded / total
    for q in range(ndet):
        piece = slice(q * part, (q + 1) * part)
        repeated = jnp.concatenate([common] * (part // period), axis=0)
        value_ref[piece] = weight_rows[piece] * (tod_all[q] - repeated)

    def late_step(i, total_sum):
        base = pl.multiple_of(i * chunk * spans, TILE)
        for span in range(spans):
            left, right = [], []
            for d in range(chunk):
                r = base + d * spans + span
                right.append(hot(low_ids, spread(low_ref, r), one))
                left.append(hot(late_ids[span], spread(high_ref, r), spread(value_ref, r)))
            total_sum = total_sum + contract(left, right)
        return total_sum

    late = lax.fori_loop(0, detectors // chunk, late_step, jnp.zeros((height, SPAN), jnp.float32))
    for p in range(peers):
        late_out[p] = late[p * TILE : (p + 1) * TILE]
    send(late_out, late_in, late_send, late_recv)
    late_in[remote] = late_out[own_place]
    early_in[remote] = early_out[own_place]

    pltpu.make_async_copy(early_in.at[pl.ds(0, remote)], early_in.at[pl.ds(0, remote)], early_recv).wait()
    first = (blk * BLK_OWN).astype(jnp.float32)

    def gather_early(n, acc):
        acc = list(acc)
        for span in range(spans):
            tile = early_in[n, span]
            label = jnp.broadcast_to(early_in[n, span, pl.ds(2 * rows, 1), :], (TILE, SPAN))
            for b in range(BLK_OWN):
                acc[b] = acc[b] + jnp.where(label == first + b, tile, 0.0)
        return tuple(acc)

    within = lax.broadcasted_iota(jnp.int32, (TILE, SPAN), 0)

    def gather_late(n, acc):
        label = jnp.broadcast_to(early_in[n, 0, pl.ds(2 * rows, 1), :], (TILE, SPAN))
        for span in range(1, spans):
            other = jnp.broadcast_to(early_in[n, span, pl.ds(2 * rows, 1), :], (TILE, SPAN))
            label = jnp.where(within < span * rows, label, other)
        tile = late_in[n]
        return tuple(
            acc[b] + jnp.where(label == first + b, tile, 0.0) for b in range(BLK_OWN)
        )

    def over_slots(step):
        acc = tuple(jnp.zeros((TILE, SPAN), jnp.float32) for _ in range(BLK_OWN))
        if total_peers <= 16:
            for n in range(total_peers):
                acc = step(n, acc)
            return acc
        return lax.fori_loop(0, total_peers, step, acc)

    acc = over_slots(gather_early)
    for b in range(BLK_OWN):
        for r in range(rows):
            at = slice(r * lanes, (r + 1) * lanes)
            out_ref[1, b : b + 1, at] = acc[b][r : r + 1, :lanes]
            out_ref[2, b : b + 1, at] = acc[b][rows + r : rows + r + 1, :lanes]

    pltpu.make_async_copy(late_in.at[pl.ds(0, remote)], late_in.at[pl.ds(0, remote)], late_recv).wait()
    acc = over_slots(gather_late)
    for b in range(BLK_OWN):
        for r in range(rows):
            line = acc[b][r : r + 1]
            for span in range(1, spans):
                line = line + acc[b][span * rows + r : span * rows + r + 1]
            out_ref[0, b : b + 1, r * lanes : (r + 1) * lanes] = line[:, :lanes]

    pltpu.make_async_copy(tod_gone, tod_all.at[pl.ds(0, ndet - 1)], tod_send).wait()
    pltpu.make_async_copy(early_in.at[pl.ds(0, remote)], early_in.at[pl.ds(0, remote)], early_send).wait()
    pltpu.make_async_copy(late_in.at[pl.ds(0, remote)], late_in.at[pl.ds(0, remote)], late_send).wait()


def on_device(tod, pixels, span_block, weight_class, class_weight):
    ndet, nblk, nsub = (lax.axis_size(a) for a in ("det", "blk", "sub"))
    mine, segments, samples = tod.shape
    detectors = pixels.shape[0]
    spans = samples // SPAN
    peers = ndet * nsub
    slots = peers * nblk
    width = BLOCK_PIX // peers
    lanes = next(n for n in range(SPAN, 0, -1) if width % n == 0)
    rows = width // lanes
    assert segments == ndet and detectors == ndet * mine
    assert TILE % spans == 0 and rows * spans <= TILE and 2 * rows < TILE
    flat = (detectors * spans, SPAN)
    vmem = pl.BlockSpec(memory_space=pltpu.VMEM)
    smem = pl.BlockSpec(memory_space=pltpu.SMEM)
    hbm = pl.BlockSpec(memory_space=pl.ANY)
    f32 = jnp.float32
    dma = pltpu.SemaphoreType.DMA
    out = pl.pallas_call(
        functools.partial(kernel, (ndet, nblk, nsub, spans, lanes, rows)),
        out_shape=pltpu.VMEM((3, BLK_OWN, width), f32),
        in_specs=[hbm, hbm, vmem, smem, smem],
        out_specs=vmem,
        scratch_shapes=[
            pltpu.VMEM(tod.shape, f32),
            pltpu.VMEM(flat, jnp.int32),
            pltpu.VMEM((ndet, mine * spans, SPAN), f32),
            pltpu.VMEM((ndet, mine * spans, SPAN), f32),
            pltpu.VMEM(flat, f32),
            pltpu.VMEM(flat, f32),
            pltpu.VMEM(flat, f32),
            pltpu.VMEM(flat, f32),
            pltpu.VMEM((peers, spans, TILE, SPAN), f32),
            pltpu.VMEM((slots, spans, TILE, SPAN), f32),
            pltpu.VMEM((peers, TILE, SPAN), f32),
            pltpu.VMEM((slots, TILE, SPAN), f32),
            dma((2,)),
            dma,
            dma,
            dma,
            dma,
            dma,
            dma,
        ],
        compiler_params=pltpu.CompilerParams(collective_id=0, has_side_effects=True),
    )(
        tod,
        pixels.reshape(flat),
        weight_class.reshape(1, detectors),
        class_weight,
        span_block.T,
    )
    return (out[0], out[1], out[2])


def solution(mesh):
    placed = (
        P(("groups", "det"), None, ("blk", "sub")),
        P("groups", "det", ("blk", "sub")),
        P("groups", ("blk", "sub")),
        P("groups"),
        P("groups"),
    )
    sliced = P(("groups", "blk"), ("det", "sub"))
    return jax.shard_map(
        on_device,
        mesh=mesh,
        in_specs=placed,
        out_specs=(sliced, sliced, sliced),
        check_vma=False,
    )
```

```python
import functools

import jax
import jax.numpy as jnp
from jax import lax
from jax.experimental import pallas as pl
from jax.experimental.pallas import tpu as pltpu
from jax.sharding import PartitionSpec as P

BLOCK_PIX = 3072
SPAN = 128
BLK_OWN = 4
TILE = 8
PACK = 16
MESH = pl.DeviceIdType.MESH


def kernel(
    sizes,
    tod_hbm,
    pix_hbm,
    class_hbm,
    class_weight_hbm,
    span_block_hbm,
    out_ref,
    class_ref,
    class_weight_ref,
    span_block_ref,
    tod_in,
    pix_in,
    stage,
    tod_all,
    high_ref,
    low_ref,
    fine_high_ref,
    fine_low_ref,
    weight_rows,
    value_ref,
    early_out,
    early_in,
    late_out,
    late_in,
    load_sem,
    tod_send,
    tod_recv,
    early_send,
    early_recv,
    late_send,
    late_recv,
    passed,
):
    ndet, nblk, nsub, spans, lanes, rows = sizes
    peers = ndet * nsub
    total_peers = peers * nblk
    mine = tod_hbm.shape[0]
    detectors = ndet * mine
    classes = class_weight_hbm.shape[0]
    det = lax.axis_index("det")
    blk = lax.axis_index("blk")
    sub = lax.axis_index("sub")
    others = [
        (db, dd, ds)
        for dd in range(ndet)
        for db in range(nblk)
        for ds in range(nsub)
        if (db, dd, ds) != (0, 0, 0)
    ]

    def target(offset):
        db, dd, ds = offset
        return {
            "det": lax.rem(det + dd, ndet),
            "blk": lax.rem(blk + db, nblk),
            "sub": lax.rem(sub + ds, nsub),
        }

    barrier = pltpu.get_barrier_semaphore()
    plane = [offset for offset in others if offset[1] == 0]
    column = [offset for offset in others if offset[0] == 0 and offset[2] == 0]
    for offset in plane + column:
        pl.semaphore_signal(barrier, inc=1, device_id=target(offset), device_id_type=MESH)

    sources = (tod_hbm, pix_hbm, class_hbm, class_weight_hbm, span_block_hbm)
    landings = (tod_in, pix_in, class_ref, class_weight_ref, span_block_ref)
    loads = [
        pltpu.make_async_copy(source, landing, load_sem.at[n])
        for n, (source, landing) in enumerate(zip(sources, landings))
    ]
    for load in loads:
        load.start()

    part = mine * spans
    loads[0].wait()
    for seg in range(ndet):
        for span in range(spans):
            stage[seg, pl.ds(span, mine, spans), :] = tod_in[:, seg, span * SPAN : (span + 1) * SPAN]
    pl.semaphore_wait(barrier, len(plane + column))
    for offset in plane:
        pl.semaphore_signal(passed, inc=1, device_id=target(offset), device_id_type=MESH)
    for step in range(1, ndet):
        seg = lax.rem(det + step, ndet)
        pltpu.make_async_remote_copy(
            src_ref=stage.at[seg],
            dst_ref=tod_all.at[det],
            send_sem=tod_send,
            recv_sem=tod_recv,
            device_id={"det": seg},
            device_id_type=MESH,
        ).start()
    tod_all[det] = stage[det]

    loads[2].wait()
    loads[3].wait()
    picked = jnp.zeros((1, detectors), jnp.float32)
    for c in range(classes):
        picked = jnp.where(class_ref[...] == c, class_weight_ref[c], picked)
    total = jnp.sum(picked, axis=1, keepdims=True)
    turned = jnp.transpose(jnp.broadcast_to(picked, (SPAN, detectors)))
    for span in range(spans):
        weight_rows[pl.ds(span, detectors, spans), :] = turned

    loads[1].wait()
    pixel = pix_in[...].astype(jnp.float32)
    high = jnp.floor((pixel + 0.5) * (1.0 / lanes))
    high_ref[...] = high
    low = pixel - high * lanes
    low_ref[...] = low
    upper = jnp.where(low >= lanes // 2, 1.0, 0.0)
    fine_high_ref[...] = 2.0 * high + upper
    fine_low_ref[...] = low - upper * (lanes // 2)

    height = peers * TILE
    fine = lanes // 2
    fine_rows = 2 * rows
    field = SPAN // spans
    low_tiles = -(-lanes // PACK)

    def iota(tile):
        return lax.broadcasted_iota(jnp.int32, (PACK, SPAN), 0) + tile * PACK

    def to_low(x):
        return x.astype(jnp.float32).astype(jnp.bfloat16)

    low_ids = [to_low(iota(t)) for t in range(SPAN // PACK)]
    early_ids = []
    late_ids = []
    for t in range(height // PACK):
        row = iota(t)
        peer = row // TILE
        within = row % TILE
        kind = jnp.where(within < rows, within, within - rows)
        early_ids.append(to_low(jnp.where(within < 2 * rows, peer * rows + kind, -1)))
    for t in range(height // PACK):
        row = iota(t)
        within = row % TILE
        late_ids.append(to_low(jnp.where(within < fine_rows, row // TILE * fine_rows + within, -1)))
    is_weight = to_low(jnp.where(iota(0) % TILE < rows, 1, 0)) > 0.5
    one = jnp.ones((PACK, SPAN), jnp.bfloat16)
    zero = jnp.zeros((PACK, SPAN), jnp.bfloat16)

    def spread(ref, row):
        return jnp.broadcast_to(ref[pl.ds(row, 1), :], (PACK, SPAN)).astype(jnp.bfloat16)

    def hot(ids, where, filled):
        return jnp.concatenate([jnp.where(i == where, filled, zero) for i in ids], axis=0)

    chunk = min(64, detectors)

    def contract(left, right):
        return lax.dot_general(
            jnp.concatenate(left, axis=1),
            jnp.concatenate(right, axis=1),
            (((1,), (1,)), ((), ())),
            preferred_element_type=jnp.float32,
        )

    def early_step(i, sums):
        base = pl.multiple_of(i * chunk * spans, TILE)
        new = []
        for span in range(spans):
            left, right = [], []
            for d in range(chunk):
                r = base + d * spans + span
                right.append(hot(low_ids, spread(low_ref, r), one))
                filled = jnp.where(is_weight, spread(weight_rows, r), one)
                left.append(hot(early_ids, spread(high_ref, r), filled))
            new.append(sums[span] + contract(left, right))
        return tuple(new)

    start = tuple(jnp.zeros((height, SPAN), jnp.float32) for _ in range(spans))
    sums = lax.fori_loop(0, detectors // chunk, early_step, start)
    loads[4].wait()
    label_row = lax.broadcasted_iota(jnp.int32, (TILE, SPAN), 0) == 2 * rows
    for span in range(spans):
        label = span_block_ref[span, det].astype(jnp.float32)
        for p in range(peers):
            tile = sums[span][p * TILE : (p + 1) * TILE]
            early_out[p, span] = jnp.where(label_row, label, tile)

    slot_of = {offset: n for n, offset in enumerate(others)}

    def send(source, landing, send_sem, recv_sem):
        for offset in others:
            to = target(offset)
            pltpu.make_async_remote_copy(
                src_ref=source.at[to["det"] * nsub + to["sub"]],
                dst_ref=landing.at[slot_of[offset]],
                send_sem=send_sem,
                recv_sem=recv_sem,
                device_id=to,
                device_id_type=MESH,
            ).start()

    own_place = det * nsub + sub
    remote = len(others)

    pl.semaphore_wait(passed, len(plane))
    send(early_out, early_in, early_send, early_recv)

    tod_gone = stage.at[pl.ds(0, ndet - 1)]
    pltpu.make_async_copy(tod_gone, tod_all.at[pl.ds(0, ndet - 1)], tod_recv).wait()

    period = TILE
    folded = jnp.zeros((period, SPAN), jnp.float32)
    for q in range(ndet):
        weighted = tod_all[q] * weight_rows[q * part : (q + 1) * part]
        for k in range(part // period):
            folded = folded + weighted[k * period : (k + 1) * period]
    shift = spans
    while shift < period:
        folded = folded + pltpu.roll(folded, shift, 0)
        shift *= 2
    common = folded / total
    for q in range(ndet):
        piece = slice(q * part, (q + 1) * part)
        repeated = jnp.concatenate([common] * (part // period), axis=0)
        value_ref[piece] = weight_rows[piece] * (tod_all[q] - repeated)

    def late_step(i, sums):
        base = pl.multiple_of(i * chunk * spans, TILE)
        new = []
        for span in range(spans):
            left, right = [], []
            for d in range(chunk):
                r = base + d * spans + span
                right.append(hot(low_ids[: field // PACK], spread(fine_low_ref, r), one))
                left.append(hot(late_ids, spread(fine_high_ref, r), spread(value_ref, r)))
            new.append(sums[span] + contract(left, right))
        return tuple(new)

    start = tuple(jnp.zeros((height, field), jnp.float32) for _ in range(spans))
    late = lax.fori_loop(0, detectors // chunk, late_step, start)
    for p in range(peers):
        tiles = [late[span][p * TILE : (p + 1) * TILE] for span in range(spans)]
        late_out[p] = jnp.concatenate(tiles, axis=1)
    send(late_out, late_in, late_send, late_recv)
    late_in[remote] = late_out[own_place]
    early_in[remote] = early_out[own_place]

    pltpu.make_async_copy(early_in.at[pl.ds(0, remote)], early_in.at[pl.ds(0, remote)], early_recv).wait()
    first = (blk * BLK_OWN).astype(jnp.float32)

    def gather_early(n, acc):
        acc = list(acc)
        for span in range(spans):
            tile = early_in[n, span]
            label = jnp.broadcast_to(early_in[n, span, pl.ds(2 * rows, 1), :], (TILE, SPAN))
            for b in range(BLK_OWN):
                acc[b] = acc[b] + jnp.where(label == first + b, tile, 0.0)
        return tuple(acc)

    lane = lax.broadcasted_iota(jnp.int32, (TILE, SPAN), 1)

    def gather_late(n, acc):
        label = jnp.broadcast_to(early_in[n, 0, pl.ds(2 * rows, 1), :], (TILE, SPAN))
        for span in range(1, spans):
            other = jnp.broadcast_to(early_in[n, span, pl.ds(2 * rows, 1), :], (TILE, SPAN))
            label = jnp.where(lane < span * field, label, other)
        tile = late_in[n]
        return tuple(
            acc[b] + jnp.where(label == first + b, tile, 0.0) for b in range(BLK_OWN)
        )

    def over_slots(step):
        acc = tuple(jnp.zeros((TILE, SPAN), jnp.float32) for _ in range(BLK_OWN))
        if total_peers <= 16:
            for n in range(total_peers):
                acc = step(n, acc)
            return acc
        return lax.fori_loop(0, total_peers, step, acc)

    acc = over_slots(gather_early)
    for b in range(BLK_OWN):
        for r in range(rows):
            at = slice(r * lanes, (r + 1) * lanes)
            out_ref[1, b : b + 1, at] = acc[b][r : r + 1, :lanes]
            out_ref[2, b : b + 1, at] = acc[b][rows + r : rows + r + 1, :lanes]

    pltpu.make_async_copy(late_in.at[pl.ds(0, remote)], late_in.at[pl.ds(0, remote)], late_recv).wait()
    acc = over_slots(gather_late)
    for b in range(BLK_OWN):
        whole = acc[b]
        for span in range(1, spans):
            whole = whole + pltpu.roll(acc[b], span * field, 1)
        for r in range(fine_rows):
            skip = r * fine % SPAN // field * field
            skip = skip if skip + fine <= SPAN else 0
            line = whole[r : r + 1, skip : skip + fine]
            out_ref[0, b : b + 1, r * fine : (r + 1) * fine] = line

    pltpu.make_async_copy(tod_gone, tod_all.at[pl.ds(0, ndet - 1)], tod_send).wait()
    pltpu.make_async_copy(early_in.at[pl.ds(0, remote)], early_in.at[pl.ds(0, remote)], early_send).wait()
    pltpu.make_async_copy(late_in.at[pl.ds(0, remote)], late_in.at[pl.ds(0, remote)], late_send).wait()


def on_device(tod, pixels, span_block, weight_class, class_weight):
    ndet, nblk, nsub = (lax.axis_size(a) for a in ("det", "blk", "sub"))
    mine, segments, samples = tod.shape
    detectors = pixels.shape[0]
    spans = samples // SPAN
    peers = ndet * nsub
    slots = peers * nblk
    width = BLOCK_PIX // peers
    lanes = next(n for n in range(SPAN, 0, -1) if width % n == 0)
    rows = width // lanes
    assert segments == ndet and detectors == ndet * mine
    assert TILE % spans == 0 and 2 * rows < TILE and lanes % 2 == 0 and lanes // 2 <= SPAN // spans
    flat = (detectors * spans, SPAN)
    vmem = pl.BlockSpec(memory_space=pltpu.VMEM)
    hbm = pl.BlockSpec(memory_space=pl.ANY)
    f32 = jnp.float32
    dma = pltpu.SemaphoreType.DMA
    out = pl.pallas_call(
        functools.partial(kernel, (ndet, nblk, nsub, spans, lanes, rows)),
        out_shape=pltpu.VMEM((3, BLK_OWN, width), f32),
        in_specs=[hbm] * 5,
        out_specs=vmem,
        scratch_shapes=[
            pltpu.VMEM((1, detectors), jnp.int32),
            pltpu.SMEM(class_weight.shape, f32),
            pltpu.SMEM((spans, segments), jnp.int32),
            pltpu.VMEM(tod.shape, f32),
            pltpu.VMEM(flat, jnp.int32),
            pltpu.VMEM((ndet, mine * spans, SPAN), f32),
            pltpu.VMEM((ndet, mine * spans, SPAN), f32),
            pltpu.VMEM(flat, f32),
            pltpu.VMEM(flat, f32),
            pltpu.VMEM(flat, f32),
            pltpu.VMEM(flat, f32),
            pltpu.VMEM(flat, f32),
            pltpu.VMEM(flat, f32),
            pltpu.VMEM((peers, spans, TILE, SPAN), f32),
            pltpu.VMEM((slots, spans, TILE, SPAN), f32),
            pltpu.VMEM((peers, TILE, SPAN), f32),
            pltpu.VMEM((slots, TILE, SPAN), f32),
            dma((5,)),
            dma,
            dma,
            dma,
            dma,
            dma,
            dma,
            pltpu.SemaphoreType.REGULAR,
        ],
        compiler_params=pltpu.CompilerParams(collective_id=0, has_side_effects=True),
    )(
        tod,
        pixels.reshape(flat),
        weight_class.reshape(1, detectors),
        class_weight,
        span_block.T,
    )
    return (out[0], out[1], out[2])


def solution(mesh):
    placed = (
        P(("groups", "det"), None, ("blk", "sub")),
        P("groups", "det", ("blk", "sub")),
        P("groups", ("blk", "sub")),
        P("groups"),
        P("groups"),
    )
    sliced = P(("groups", "blk"), ("det", "sub"))
    return jax.shard_map(
        on_device,
        mesh=mesh,
        in_specs=placed,
        out_specs=(sliced, sliced, sliced),
        check_vma=False,
    )
```

```python
import functools

import jax
import jax.numpy as jnp
from jax import lax
from jax.experimental import pallas as pl
from jax.experimental.pallas import tpu as pltpu
from jax.sharding import PartitionSpec as P

BLOCK_PIX = 3072
SPAN = 128
BLK_OWN = 4
TILE = 8
PACK = 16
MESH = pl.DeviceIdType.MESH


def kernel(
    sizes,
    tod_hbm,
    pix_hbm,
    class_hbm,
    class_weight_hbm,
    span_block_hbm,
    out_ref,
    class_ref,
    class_weight_ref,
    span_block_ref,
    tod_in,
    pix_in,
    stage,
    tod_all,
    high_ref,
    low_ref,
    fine_high_ref,
    fine_low_ref,
    weight_rows,
    value_ref,
    early_out,
    early_in,
    late_out,
    late_in,
    load_sem,
    tod_send,
    tod_recv,
    early_send,
    early_recv,
    late_send,
    late_recv,
    passed,
):
    ndet, nblk, nsub, spans, lanes, rows = sizes
    peers = ndet * nsub
    total_peers = peers * nblk
    mine = tod_hbm.shape[0]
    detectors = ndet * mine
    classes = class_weight_hbm.shape[0]
    det = lax.axis_index("det")
    blk = lax.axis_index("blk")
    sub = lax.axis_index("sub")
    others = [
        (db, dd, ds)
        for dd in range(ndet)
        for db in range(nblk)
        for ds in range(nsub)
        if (db, dd, ds) != (0, 0, 0)
    ]

    def target(offset):
        db, dd, ds = offset
        return {
            "det": lax.rem(det + dd, ndet),
            "blk": lax.rem(blk + db, nblk),
            "sub": lax.rem(sub + ds, nsub),
        }

    barrier = pltpu.get_barrier_semaphore()
    plane = [offset for offset in others if offset[1] == 0]
    column = [offset for offset in others if offset[0] == 0 and offset[2] == 0]
    for offset in plane + column:
        pl.semaphore_signal(barrier, inc=1, device_id=target(offset), device_id_type=MESH)

    sources = (tod_hbm, pix_hbm, class_hbm, class_weight_hbm, span_block_hbm)
    landings = (tod_in, pix_in, class_ref, class_weight_ref, span_block_ref)
    loads = [
        pltpu.make_async_copy(source, landing, load_sem.at[n])
        for n, (source, landing) in enumerate(zip(sources, landings))
    ]
    for load in loads:
        load.start()

    part = mine * spans
    loads[0].wait()
    for seg in range(ndet):
        for span in range(spans):
            stage[seg, pl.ds(span, mine, spans), :] = tod_in[:, seg, span * SPAN : (span + 1) * SPAN]

    loads[2].wait()
    loads[3].wait()
    picked = jnp.zeros((1, detectors), jnp.float32)
    for c in range(classes):
        picked = jnp.where(class_ref[...] == c, class_weight_ref[c], picked)
    total = jnp.sum(picked, axis=1, keepdims=True)
    turned = jnp.transpose(jnp.broadcast_to(picked, (SPAN, detectors)))
    for span in range(spans):
        weight_rows[pl.ds(span, detectors, spans), :] = turned

    loads[1].wait()
    pixel = pix_in[...].astype(jnp.float32)
    high = jnp.floor((pixel + 0.5) * (1.0 / lanes))
    high_ref[...] = high
    low = pixel - high * lanes
    low_ref[...] = low
    upper = jnp.where(low >= lanes // 2, 1.0, 0.0)
    fine_high_ref[...] = 2.0 * high + upper
    fine_low_ref[...] = low - upper * (lanes // 2)

    pl.semaphore_wait(barrier, len(plane + column))
    for offset in plane:
        pl.semaphore_signal(passed, inc=1, device_id=target(offset), device_id_type=MESH)
    for step in range(1, ndet):
        seg = lax.rem(det + step, ndet)
        pltpu.make_async_remote_copy(
            src_ref=stage.at[seg],
            dst_ref=tod_all.at[det],
            send_sem=tod_send,
            recv_sem=tod_recv,
            device_id={"det": seg},
            device_id_type=MESH,
        ).start()
    tod_all[det] = stage[det]
    height = peers * TILE
    fine = lanes // 2
    fine_rows = 2 * rows
    field = SPAN // spans
    low_tiles = -(-lanes // PACK)

    def iota(tile):
        return lax.broadcasted_iota(jnp.int32, (PACK, SPAN), 0) + tile * PACK

    def to_low(x):
        return x.astype(jnp.float32).astype(jnp.bfloat16)

    low_ids = [to_low(iota(t)) for t in range(SPAN // PACK)]
    early_ids = []
    late_ids = []
    for t in range(height // PACK):
        row = iota(t)
        peer = row // TILE
        within = row % TILE
        kind = jnp.where(within < rows, within, within - rows)
        early_ids.append(to_low(jnp.where(within < 2 * rows, peer * rows + kind, -1)))
    for t in range(height // PACK):
        row = iota(t)
        within = row % TILE
        late_ids.append(to_low(jnp.where(within < fine_rows, row // TILE * fine_rows + within, -1)))
    is_weight = to_low(jnp.where(iota(0) % TILE < rows, 1, 0)) > 0.5
    one = jnp.ones((PACK, SPAN), jnp.bfloat16)
    zero = jnp.zeros((PACK, SPAN), jnp.bfloat16)

    def spread(ref, row):
        return jnp.broadcast_to(ref[pl.ds(row, 1), :], (PACK, SPAN)).astype(jnp.bfloat16)

    def hot(ids, where, filled):
        return jnp.concatenate([jnp.where(i == where, filled, zero) for i in ids], axis=0)

    chunk = min(64, detectors)

    def contract(left, right):
        return lax.dot_general(
            jnp.concatenate(left, axis=1),
            jnp.concatenate(right, axis=1),
            (((1,), (1,)), ((), ())),
            preferred_element_type=jnp.float32,
        )

    def early_step(i, sums):
        base = pl.multiple_of(i * chunk * spans, TILE)
        new = []
        for span in range(spans):
            left, right = [], []
            for d in range(chunk):
                r = base + d * spans + span
                right.append(hot(low_ids, spread(low_ref, r), one))
                filled = jnp.where(is_weight, spread(weight_rows, r), one)
                left.append(hot(early_ids, spread(high_ref, r), filled))
            new.append(sums[span] + contract(left, right))
        return tuple(new)

    start = tuple(jnp.zeros((height, SPAN), jnp.float32) for _ in range(spans))
    sums = lax.fori_loop(0, detectors // chunk, early_step, start)
    loads[4].wait()
    label_row = lax.broadcasted_iota(jnp.int32, (TILE, SPAN), 0) == 2 * rows
    for span in range(spans):
        label = span_block_ref[span, det].astype(jnp.float32)
        for p in range(peers):
            tile = sums[span][p * TILE : (p + 1) * TILE]
            early_out[p, span] = jnp.where(label_row, label, tile)

    slot_of = {offset: n for n, offset in enumerate(others)}

    def send(source, landing, send_sem, recv_sem):
        for offset in others:
            to = target(offset)
            pltpu.make_async_remote_copy(
                src_ref=source.at[to["det"] * nsub + to["sub"]],
                dst_ref=landing.at[slot_of[offset]],
                send_sem=send_sem,
                recv_sem=recv_sem,
                device_id=to,
                device_id_type=MESH,
            ).start()

    own_place = det * nsub + sub
    remote = len(others)

    pl.semaphore_wait(passed, len(plane))
    send(early_out, early_in, early_send, early_recv)

    tod_gone = stage.at[pl.ds(0, ndet - 1)]
    pltpu.make_async_copy(tod_gone, tod_all.at[pl.ds(0, ndet - 1)], tod_recv).wait()

    period = TILE
    folded = jnp.zeros((period, SPAN), jnp.float32)
    for q in range(ndet):
        weighted = tod_all[q] * weight_rows[q * part : (q + 1) * part]
        for k in range(part // period):
            folded = folded + weighted[k * period : (k + 1) * period]
    shift = spans
    while shift < period:
        folded = folded + pltpu.roll(folded, shift, 0)
        shift *= 2
    common = folded / total
    for q in range(ndet):
        piece = slice(q * part, (q + 1) * part)
        repeated = jnp.concatenate([common] * (part // period), axis=0)
        value_ref[piece] = weight_rows[piece] * (tod_all[q] - repeated)

    def late_step(i, sums):
        base = pl.multiple_of(i * chunk * spans, TILE)
        new = []
        for span in range(spans):
            left, right = [], []
            for d in range(chunk):
                r = base + d * spans + span
                right.append(hot(low_ids[: field // PACK], spread(fine_low_ref, r), one))
                left.append(hot(late_ids, spread(fine_high_ref, r), spread(value_ref, r)))
            new.append(sums[span] + contract(left, right))
        return tuple(new)

    start = tuple(jnp.zeros((height, field), jnp.float32) for _ in range(spans))
    late = lax.fori_loop(0, detectors // chunk, late_step, start)
    for p in range(peers):
        tiles = [late[span][p * TILE : (p + 1) * TILE] for span in range(spans)]
        late_out[p] = jnp.concatenate(tiles, axis=1)
    send(late_out, late_in, late_send, late_recv)
    late_in[remote] = late_out[own_place]
    early_in[remote] = early_out[own_place]

    pltpu.make_async_copy(early_in.at[pl.ds(0, remote)], early_in.at[pl.ds(0, remote)], early_recv).wait()
    first = (blk * BLK_OWN).astype(jnp.float32)

    def gather_early(n, acc):
        acc = list(acc)
        for span in range(spans):
            tile = early_in[n, span]
            label = jnp.broadcast_to(early_in[n, span, pl.ds(2 * rows, 1), :], (TILE, SPAN))
            for b in range(BLK_OWN):
                acc[b] = acc[b] + jnp.where(label == first + b, tile, 0.0)
        return tuple(acc)

    lane = lax.broadcasted_iota(jnp.int32, (TILE, SPAN), 1)

    def gather_late(n, acc):
        label = jnp.broadcast_to(early_in[n, 0, pl.ds(2 * rows, 1), :], (TILE, SPAN))
        for span in range(1, spans):
            other = jnp.broadcast_to(early_in[n, span, pl.ds(2 * rows, 1), :], (TILE, SPAN))
            label = jnp.where(lane < span * field, label, other)
        tile = late_in[n]
        return tuple(
            acc[b] + jnp.where(label == first + b, tile, 0.0) for b in range(BLK_OWN)
        )

    def over_slots(step):
        acc = tuple(jnp.zeros((TILE, SPAN), jnp.float32) for _ in range(BLK_OWN))
        if total_peers <= 16:
            for n in range(total_peers):
                acc = step(n, acc)
            return acc
        return lax.fori_loop(0, total_peers, step, acc)

    acc = over_slots(gather_early)
    for b in range(BLK_OWN):
        for r in range(rows):
            at = slice(r * lanes, (r + 1) * lanes)
            out_ref[1, b : b + 1, at] = acc[b][r : r + 1, :lanes]
            out_ref[2, b : b + 1, at] = acc[b][rows + r : rows + r + 1, :lanes]

    pltpu.make_async_copy(late_in.at[pl.ds(0, remote)], late_in.at[pl.ds(0, remote)], late_recv).wait()
    acc = over_slots(gather_late)
    for b in range(BLK_OWN):
        whole = acc[b]
        for span in range(1, spans):
            whole = whole + pltpu.roll(acc[b], span * field, 1)
        for r in range(fine_rows):
            skip = r * fine % SPAN // field * field
            skip = skip if skip + fine <= SPAN else 0
            line = whole[r : r + 1, skip : skip + fine]
            out_ref[0, b : b + 1, r * fine : (r + 1) * fine] = line

    pltpu.make_async_copy(tod_gone, tod_all.at[pl.ds(0, ndet - 1)], tod_send).wait()
    pltpu.make_async_copy(early_in.at[pl.ds(0, remote)], early_in.at[pl.ds(0, remote)], early_send).wait()
    pltpu.make_async_copy(late_in.at[pl.ds(0, remote)], late_in.at[pl.ds(0, remote)], late_send).wait()


def on_device(tod, pixels, span_block, weight_class, class_weight):
    ndet, nblk, nsub = (lax.axis_size(a) for a in ("det", "blk", "sub"))
    mine, segments, samples = tod.shape
    detectors = pixels.shape[0]
    spans = samples // SPAN
    peers = ndet * nsub
    slots = peers * nblk
    width = BLOCK_PIX // peers
    lanes = next(n for n in range(SPAN, 0, -1) if width % n == 0)
    rows = width // lanes
    assert segments == ndet and detectors == ndet * mine
    assert TILE % spans == 0 and 2 * rows < TILE and lanes % 2 == 0 and lanes // 2 <= SPAN // spans
    flat = (detectors * spans, SPAN)
    vmem = pl.BlockSpec(memory_space=pltpu.VMEM)
    hbm = pl.BlockSpec(memory_space=pl.ANY)
    f32 = jnp.float32
    dma = pltpu.SemaphoreType.DMA
    out = pl.pallas_call(
        functools.partial(kernel, (ndet, nblk, nsub, spans, lanes, rows)),
        out_shape=pltpu.VMEM((3, BLK_OWN, width), f32),
        in_specs=[hbm] * 5,
        out_specs=vmem,
        scratch_shapes=[
            pltpu.VMEM((1, detectors), jnp.int32),
            pltpu.SMEM(class_weight.shape, f32),
            pltpu.SMEM((spans, segments), jnp.int32),
            pltpu.VMEM(tod.shape, f32),
            pltpu.VMEM(flat, jnp.int32),
            pltpu.VMEM((ndet, mine * spans, SPAN), f32),
            pltpu.VMEM((ndet, mine * spans, SPAN), f32),
            pltpu.VMEM(flat, f32),
            pltpu.VMEM(flat, f32),
            pltpu.VMEM(flat, f32),
            pltpu.VMEM(flat, f32),
            pltpu.VMEM(flat, f32),
            pltpu.VMEM(flat, f32),
            pltpu.VMEM((peers, spans, TILE, SPAN), f32),
            pltpu.VMEM((slots, spans, TILE, SPAN), f32),
            pltpu.VMEM((peers, TILE, SPAN), f32),
            pltpu.VMEM((slots, TILE, SPAN), f32),
            dma((5,)),
            dma,
            dma,
            dma,
            dma,
            dma,
            dma,
            pltpu.SemaphoreType.REGULAR,
        ],
        compiler_params=pltpu.CompilerParams(collective_id=0, has_side_effects=True),
    )(
        tod,
        pixels.reshape(flat),
        weight_class.reshape(1, detectors),
        class_weight,
        span_block.T,
    )
    return (out[0], out[1], out[2])


def solution(mesh):
    placed = (
        P(("groups", "det"), None, ("blk", "sub")),
        P("groups", "det", ("blk", "sub")),
        P("groups", ("blk", "sub")),
        P("groups"),
        P("groups"),
    )
    sliced = P(("groups", "blk"), ("det", "sub"))
    return jax.shard_map(
        on_device,
        mesh=mesh,
        in_specs=placed,
        out_specs=(sliced, sliced, sliced),
        check_vma=False,
    )
```
